32 devices in a mesh: head: 2 (over y), blk: 16 (over z, x, core).
Axes of the slice: x: 2, y: 2, z: 4, core: 2. Of those that a mesh axis runs over, the one named last changes fastest.
Arguments:
- query_rows: bfloat16 [16, 144, 3072], P('blk', 'head'), may hold values from -6 to 6
- key_rows: bfloat16 [16, 144, 3072], P('blk', 'head'), may hold values from -6 to 6
- value_rows: bfloat16 [16, 144, 3072], P('blk', 'head'), may hold values from -6 to 6
- query_tangent: bfloat16 [16, 144, 3072], P('blk', 'head'), may hold values from -6 to 6
- key_tangent: bfloat16 [16, 144, 3072], P('blk', 'head'), may hold values from -6 to 6
- value_tangent: bfloat16 [16, 144, 3072], P('blk', 'head'), may hold values from -6 to 6
- query_gain: float32 [128], replicated, may hold values from 1 to 6
- key_gain: float32 [128], replicated, may hold values from 1 to 6
Outputs:
- attended: bfloat16 [16, 144, 3072], P('blk', 'head')
- attended_tangent: bfloat16 [16, 144, 3072], P('blk', 'head')
The draws below stay inside these ranges and needn't reach their ends.
All inputs are finite; a program needn't handle non-finite values.
Results may differ from the reference program's by a relative error of at most 0.014.
The reference program's roundings to bfloat16 on the way count: a program that leaves them out, or rounds other values in their place, can miss the bound.
Values may be sent and summed in bfloat16 or wider, within the bound.
No kernel may reach another device: no remote copies, remote signals or barrier semaphores. Data moves between devices by JAX's collectives and lax.ppermute only.
A program may use at most 64 MiB of HBM per device.

```python
import math
import jax
import jax.numpy as jnp
from jax import lax

HEADS = 24
HD = 128
D = 3072
TXT = 512
GRID_W = 64
GROUP = 16
ROWS = 144
IMAGES = 1
SEQ = 2304
BLOCKS = 16


def joint_pair(key):
    shape = (IMAGES, SEQ, D)
    key_values = jax.random.normal(jax.random.fold_in(key, 101), shape, jnp.float32)
    query_values = jax.random.normal(jax.random.fold_in(key, 102), shape, jnp.float32)

    def blocked(feature_field):
        feature_field = jnp.clip(feature_field, -6.0, 6.0).reshape(IMAGES, GROUP, ROWS, D)
        return feature_field.transpose(1, 0, 2, 3).reshape(GROUP * IMAGES, ROWS, D).astype(jnp.bfloat16)
    return (blocked(query_values), blocked(key_values))


def gain_draw(key):
    return jnp.exp(jax.random.uniform(key, (HD,), jnp.float32, 0.0, jnp.log(2.2)))


def draw_query_rows(key, part):
    return joint_pair(key)[0]


def draw_key_rows(key, part):
    return joint_pair(key)[1]


def draw_query_gain(key, part):
    return gain_draw(jax.random.fold_in(key, 201))


def draw_key_gain(key, part):
    return gain_draw(jax.random.fold_in(key, 202))


def level_of(own_key, extent, shards, least, top_value):
    factor_of = 1.0
    for dim, blocks in shards:
        heights = jax.random.uniform(jax.random.fold_in(jax.random.fold_in(own_key, 6), dim), (blocks,), jnp.float32, least / len(shards), top_value / len(shards))
        factor_of = factor_of * jnp.repeat(jnp.exp(heights), extent[dim] // blocks).reshape((-1,) + (1,) * (len(extent) - 1 - dim))
    return factor_of


def normal_values(own_key, dims, spread, bound, shards=(), held_as=jnp.bfloat16):
    loudness = level_of(own_key, dims, shards, -0.22, 0.18) if shards else 1.0
    values = jax.random.normal(own_key, dims, jnp.float32) * spread * loudness
    return jnp.minimum(jnp.maximum(values, -bound), bound).astype(held_as)


def setup_inputs(seed: int = 0) -> dict:
    key_of = jax.random.split(jax.random.key(seed), 9)
    query_rows = draw_query_rows(jax.random.fold_in(key_of[8], 71), 0)
    key_rows = draw_key_rows(jax.random.fold_in(key_of[8], 71), 0)
    value_rows = normal_values(key_of[2], (BLOCKS, ROWS, D), 1.0, 6.0, ((0, 16), (1, 2)))
    query_tangent = normal_values(key_of[3], (BLOCKS, ROWS, D), 1.0, 6.0, ((0, 16), (1, 2)))
    key_tangent = normal_values(key_of[4], (BLOCKS, ROWS, D), 1.0, 6.0, ((0, 16), (1, 2)))
    value_tangent = normal_values(key_of[5], (BLOCKS, ROWS, D), 1.0, 6.0, ((0, 16), (1, 2)))
    query_gain = draw_query_gain(jax.random.fold_in(key_of[8], 71), 0)
    key_gain = draw_key_gain(jax.random.fold_in(key_of[8], 71), 0)
    return {"query_rows": query_rows, "key_rows": key_rows, "value_rows": value_rows, "query_tangent": query_tangent, "key_tangent": key_tangent, "value_tangent": value_tangent, "query_gain": query_gain, "key_gain": key_gain}


EPSILON = 1e-06
THETA = 10000.0

def rotation(first, count, head_dim):
    block_offsets = first + jnp.arange(count, dtype=jnp.int32)
    is_image = block_offsets >= TXT
    patch = jnp.maximum(block_offsets - TXT, 0)
    row_id = jnp.where(is_image, patch // GRID_W, 0).astype(jnp.float32)
    column_id = jnp.where(is_image, patch % GRID_W, 0).astype(jnp.float32)
    leading = head_dim // 8
    lateral = (head_dim - leading) // 2
    exponent = jnp.arange(lateral // 2, dtype=jnp.float32) * (2.0 / lateral)
    frequency = jnp.exp(-math.log(THETA) * exponent)
    angles = jnp.concatenate([jnp.zeros((count, leading // 2), jnp.float32), row_id[:, None] * frequency[None, :], column_id[:, None] * frequency[None, :]], axis=1)
    angles = jnp.repeat(angles, 2, axis=1)
    return (jnp.cos(angles), jnp.sin(angles))

def rotation_partner(head_dim):
    across = jnp.arange(head_dim, dtype=jnp.int32)
    lower = across[:, None]
    upper = across[None, :]
    forward = ((upper == lower + 1) & (lower % 2 == 0)).astype(jnp.float32)
    backward = ((lower == upper + 1) & (upper % 2 == 0)).astype(jnp.float32)
    return forward - backward

def normalize(raw, tangent, gain, cosine, sine, partner):
    values = raw.astype(jnp.float32)
    motion = tangent.astype(jnp.float32)
    inverse = lax.rsqrt(lax.optimization_barrier(jnp.mean(values * values, axis=-1, keepdims=True)) + EPSILON)
    coupling = lax.optimization_barrier(jnp.mean(values * motion, axis=-1, keepdims=True))
    normed = values * inverse * gain
    normalized_tangent = gain * (motion * inverse - values * inverse * inverse * inverse * coupling)

    def rotate(feature_field):
        return feature_field * cosine + jnp.dot(feature_field, partner, precision=lax.Precision.HIGHEST) * sine
    return (rotate(normed).astype(jnp.bfloat16), rotate(normalized_tangent).astype(jnp.bfloat16))

def attend(item):
    query_hat, query_dot, key_hat, key_dot, value, value_dot = [feature_field.astype(jnp.float32) for feature_field in item]
    scale = 1.0 / math.sqrt(HD)
    logit_scores = jnp.dot(query_hat, key_hat.T, preferred_element_type=jnp.float32) * scale
    peak = lax.optimization_barrier(jnp.max(logit_scores, axis=1, keepdims=True))
    weights = jnp.exp(logit_scores - peak)
    total = lax.optimization_barrier(jnp.sum(weights, axis=1, keepdims=True))
    score_dot = (jnp.dot(query_dot, key_hat.T, preferred_element_type=jnp.float32) + jnp.dot(query_hat, key_dot.T, preferred_element_type=jnp.float32)) * scale
    product = weights * score_dot
    drift = lax.optimization_barrier(jnp.sum(product, axis=1, keepdims=True))
    low_weights = lax.optimization_barrier(weights.astype(jnp.bfloat16)).astype(jnp.float32)
    low_product = lax.optimization_barrier(product.astype(jnp.bfloat16)).astype(jnp.float32)
    summed = jnp.dot(low_weights, value, preferred_element_type=jnp.float32)
    summed_dot = jnp.dot(low_weights, value_dot, preferred_element_type=jnp.float32) + jnp.dot(low_product, value, preferred_element_type=jnp.float32)
    attention_output = (summed / total).astype(jnp.bfloat16)
    output_tangent = ((summed_dot - drift / total * summed) / total).astype(jnp.bfloat16)
    return (attention_output, output_tangent)

def reference(query_rows, key_rows, value_rows, query_tangent, key_tangent, value_tangent, query_gain, key_gain):

    def unblock(blocked):
        return blocked.reshape(GROUP, IMAGES, ROWS, HEADS, HD).transpose(1, 0, 2, 3, 4).reshape(IMAGES, SEQ, HEADS, HD)
    cosine, sine = rotation(0, SEQ, HD)
    cosine = cosine[None, :, None, :]
    sine = sine[None, :, None, :]
    partner = rotation_partner(HD)
    query_hat, query_dot = normalize(unblock(query_rows), unblock(query_tangent), query_gain, cosine, sine, partner)
    key_hat, key_dot = normalize(unblock(key_rows), unblock(key_tangent), key_gain, cosine, sine, partner)

    def per_head_split(feature_field):
        return feature_field.transpose(0, 2, 1, 3).reshape(IMAGES * HEADS, SEQ, HD)
    items = tuple((per_head_split(feature_field) for feature_field in (query_hat, query_dot, key_hat, key_dot, unblock(value_rows), unblock(value_tangent))))
    attention_output, output_tangent = lax.map(attend, items)

    def regroup_blocks(feature_field):
        feature_field = feature_field.reshape(IMAGES, HEADS, SEQ, HD).transpose(0, 2, 1, 3)
        feature_field = feature_field.reshape(IMAGES, GROUP, ROWS, HEADS * HD).transpose(1, 0, 2, 3)
        return feature_field.reshape(GROUP * IMAGES, ROWS, HEADS * HD)
    return (regroup_blocks(attention_output), regroup_blocks(output_tangent))
```

```python
import functools
import math

import jax
import jax.numpy as jnp
from jax import lax
from jax.experimental import pallas as pl
from jax.experimental.pallas import tpu as pltpu
from jax.sharding import PartitionSpec as P

HD = 128
TXT = 512
GRID_W = 64
GROUP = 16
EPSILON = 1e-06
THETA = 10000.0
LOG2E = math.log2(math.e)
MASKED = -1e30


def rotation(first, count, head_dim):
    tokens = first + jnp.arange(count, dtype=jnp.int32)
    is_image = tokens >= TXT
    patch = jnp.maximum(tokens - TXT, 0)
    row_id = jnp.where(is_image, patch // GRID_W, 0).astype(jnp.float32)[:, None]
    column_id = jnp.where(is_image, patch % GRID_W, 0).astype(jnp.float32)[:, None]
    leading = head_dim // 8
    lateral = (head_dim - leading) // 2
    lane = jnp.arange(head_dim, dtype=jnp.int32)
    by_row = (lane >= leading) & (lane < leading + lateral)
    by_column = lane >= leading + lateral
    offset = jnp.where(by_row, lane - leading, jnp.where(by_column, lane - leading - lateral, 0))
    exponent = (offset // 2).astype(jnp.float32) * (2.0 / lateral)
    frequency = jnp.exp(-math.log(THETA) * exponent)
    angles = jnp.where(by_row, row_id, jnp.where(by_column, column_id, 0.0)) * frequency
    sine = jnp.where(lane % 2 == 0, -jnp.sin(angles), jnp.sin(angles))
    return jnp.cos(angles), sine


def prepare_body(where, q_ref, k_ref, v_ref, qt_ref, kt_ref, vt_ref, gain_ref, turn_ref, q_out, kv_out):
    heads = kv_out.shape[1]
    cosine = turn_ref[0]
    sine = turn_ref[1]
    even = lax.broadcasted_iota(jnp.int32, cosine.shape, 1) % 2 == 0

    def rotate(x):
        partner = jnp.where(even, pltpu.roll(x, HD - 1, 1), pltpu.roll(x, 1, 1))
        return x * cosine + partner * sine

    def normalize(raw, tangent, gain):
        values = raw.astype(jnp.float32)
        motion = tangent.astype(jnp.float32)
        inverse = lax.rsqrt(jnp.mean(values * values, axis=-1, keepdims=True) + EPSILON)
        coupling = jnp.mean(values * motion, axis=-1, keepdims=True)
        normed = values * inverse
        moved = motion * inverse - normed * (inverse * inverse * coupling)
        return rotate(normed * gain).astype(jnp.bfloat16), rotate(moved * gain).astype(jnp.bfloat16)

    for h in range(heads):
        lanes = slice(h * HD, (h + 1) * HD)
        hat, dot = normalize(q_ref[0, :, lanes], qt_ref[0, :, lanes], gain_ref[0:1])
        q_out[0, h] = dot
        q_out[1, h] = hat
        hat, dot = normalize(k_ref[0, :, lanes], kt_ref[0, :, lanes], gain_ref[1:2])
        kv_out[0, h] = hat
        kv_out[1, h] = dot
        kv_out[2, h] = v_ref[0, :, lanes]
        kv_out[3, h] = vt_ref[0, :, lanes]


def prepare(group, mask, args, gains, turn, heads):
    rows = args[0].shape[1]
    width = heads * HD
    column = pl.BlockSpec((1, rows, width), lambda i, where: (0, 0, where[0] ^ mask))
    return pl.pallas_call(
        prepare_body,
        grid_spec=pltpu.PrefetchScalarGridSpec(
            num_scalar_prefetch=1,
            grid=(1,),
            in_specs=[column] * 6
            + [
                pl.BlockSpec((2, HD), lambda i, where: (0, 0)),
                pl.BlockSpec((2, rows, HD), lambda i, where: (0, 0, 0)),
            ],
            out_specs=[
                pl.BlockSpec((2, heads, rows, HD), lambda i, where: (0, 0, 0, 0)),
                pl.BlockSpec((4, heads, rows, HD), lambda i, where: (0, 0, 0, 0)),
            ],
        ),
        out_shape=[
            jax.ShapeDtypeStruct((2, heads, rows, HD), jnp.bfloat16),
            jax.ShapeDtypeStruct((4, heads, rows, HD), jnp.bfloat16),
        ],
        compiler_params=pltpu.CompilerParams(vmem_limit_bytes=8 << 20),
        cost_estimate=pl.CostEstimate(
            flops=40 * 4 * heads * rows * HD, bytes_accessed=24 * heads * rows * HD, transcendentals=heads * rows
        ),
        name="prepare",
    )(group, *args, gains, turn)


def attend_body(pieces_q, pieces, first, last, block, *refs):
    refs = list(refs)
    take = lambda n: [refs.pop(0) for _ in range(n)]
    q_in = take(pieces_q)
    kv = take(pieces)
    if not first:
        acc_in, stat_in = take(2)
    if first and not last:
        (q_out,) = take(1)
    if last:
        outs = take(len(refs) - 3)
    else:
        acc_out, stat_out = take(2)
    q_all, k_all, v_all = refs
    rows = q_all.shape[0]
    count = k_all.shape[0]

    def joined(parts, a):
        return jnp.concatenate([p[a, 0] for p in parts], axis=0)

    if first:
        q_all[:, :HD] = joined(q_in, 0)
        q_all[:, HD:] = joined(q_in, 1)
        if not last:
            q_out[0] = q_all[...]
        queries = q_all
    else:
        queries = q_in[0].at[0]
    k_all[:, :HD] = joined(kv, 0)
    k_all[:, HD:] = joined(kv, 1)
    v_all[:, :HD] = joined(kv, 2)
    v_all[:, HD:] = joined(kv, 3)
    scale = 1.0 / math.sqrt(HD)
    contract = (((1,), (1,)), ((), ()))
    lane = lax.broadcasted_iota(jnp.int32, (block, HD), 1)

    def step(i, _):
        span = pl.ds(pl.multiple_of(i * block, block), block)
        pair = queries[span, :]
        logits = lax.dot_general(pair[:, HD:], k_all[:, :HD], contract, preferred_element_type=jnp.float32)
        moved = lax.dot_general(pair, k_all[...], contract, preferred_element_type=jnp.float32)
        peak = jnp.max(logits, axis=1, keepdims=True)
        if not first:
            stat = stat_in[0, span, :]
            before = stat[:, 0:1]
            peak = jnp.maximum(peak, before)
            fade = jnp.exp2((before - peak) * (scale * LOG2E))
        weights = jnp.exp2((logits - peak) * (scale * LOG2E))
        product = weights * (moved * scale)
        total = jnp.sum(weights, axis=1, keepdims=True)
        drift = jnp.sum(product, axis=1, keepdims=True)
        both = jnp.dot(weights.astype(jnp.bfloat16), v_all[...], preferred_element_type=jnp.float32)
        other = jnp.dot(product.astype(jnp.bfloat16), v_all[:, :HD], preferred_element_type=jnp.float32)
        summed = both[:, :HD]
        summed_dot = both[:, HD:] + other
        if not first:
            total = total + fade * stat[:, 1:2]
            drift = drift + fade * stat[:, 2:3]
            summed = summed + fade * acc_in[0, span, :HD]
            summed_dot = summed_dot + fade * acc_in[0, span, HD:]
        if last:
            inverse = 1.0 / total
            q_all[span, :HD] = (summed * inverse).astype(jnp.bfloat16)
            q_all[span, HD:] = ((summed_dot - (drift * inverse) * summed) * inverse).astype(jnp.bfloat16)
        else:
            acc_out[0, span, :HD] = summed
            acc_out[0, span, HD:] = summed_dot
            stat_out[0, span, :] = jnp.where(lane == 0, peak, jnp.where(lane == 1, total, drift))
        return 0

    lax.fori_loop(0, rows // block, step, 0)
    if last:
        each = rows // len(outs)
        for n, out in enumerate(outs):
            out[0, 0] = q_all[n * each : (n + 1) * each, :HD]
            out[1, 0] = q_all[n * each : (n + 1) * each, HD:]


def attend(q_in, kv, state, last, returns):
    first = state is None
    heads = kv[0].shape[1]
    count = sum(b.shape[2] for b in kv)
    rows = sum(b.shape[2] for b in q_in) if first else q_in[0].shape[1]
    block = max(b for b in range(8, 193, 8) if rows % b == 0)

    def head_spec(b):
        return pl.BlockSpec((b.shape[0], 1, b.shape[2], HD), lambda h: (0, h, 0, 0))

    full = pl.BlockSpec((1, rows, 2 * HD), lambda h: (h, 0, 0))
    stat = pl.BlockSpec((1, rows, HD), lambda h: (h, 0, 0))
    in_specs = [head_spec(b) for b in q_in] if first else [full]
    in_specs += [head_spec(b) for b in kv]
    operands = list(q_in) + list(kv)
    if not first:
        in_specs += [full, stat]
        operands += list(state)
    out_specs, out_shape = [], []
    if first and not last:
        out_specs.append(full)
        out_shape.append(jax.ShapeDtypeStruct((heads, rows, 2 * HD), jnp.bfloat16))
    if last:
        shape = (2, heads, rows // returns, HD)
        out_specs += [pl.BlockSpec((2, 1, rows // returns, HD), lambda h: (0, h, 0, 0))] * returns
        out_shape += [jax.ShapeDtypeStruct(shape, jnp.bfloat16)] * returns
    else:
        out_specs += [full, stat]
        out_shape += [
            jax.ShapeDtypeStruct((heads, rows, 2 * HD), jnp.float32),
            jax.ShapeDtypeStruct((heads, rows, HD), jnp.float32),
        ]
    return pl.pallas_call(
        functools.partial(attend_body, len(q_in), len(kv), first, last, block),
        grid=(heads,),
        in_specs=in_specs,
        out_specs=out_specs,
        out_shape=out_shape,
        scratch_shapes=[
            pltpu.VMEM((rows, 2 * HD), jnp.bfloat16),
            pltpu.VMEM((count, 2 * HD), jnp.bfloat16),
            pltpu.VMEM((count, 2 * HD), jnp.bfloat16),
        ],
        compiler_params=pltpu.CompilerParams(vmem_limit_bytes=32 << 20),
        cost_estimate=pl.CostEstimate(
            flops=12 * heads * rows * count * HD,
            bytes_accessed=8 * heads * count * HD + 4 * heads * rows * HD,
            transcendentals=heads * rows * count,
        ),
        name="attend",
    )(*operands)


def assemble_body(where, *refs):
    *parts, out, out_tangent = refs
    heads = parts[0].shape[1]
    for mask, part in enumerate(parts):
        column = (where[0] ^ mask) * (heads * HD)
        for h in range(heads):
            lanes = pl.ds(pl.multiple_of(column + h * HD, HD), HD)
            out[0, :, lanes] = part[0, h]
            out_tangent[0, :, lanes] = part[1, h]


def assemble(group, parts):
    _, heads, rows, _ = parts[0].shape
    shape = (1, rows, len(parts) * heads * HD)
    return pl.pallas_call(
        assemble_body,
        in_specs=[pl.BlockSpec(memory_space=pltpu.SMEM)] + [pl.BlockSpec(memory_space=pltpu.VMEM)] * len(parts),
        out_specs=[pl.BlockSpec(memory_space=pltpu.VMEM)] * 2,
        out_shape=[jax.ShapeDtypeStruct(shape, jnp.bfloat16)] * 2,
        compiler_params=pltpu.CompilerParams(vmem_limit_bytes=8 << 20),
        name="assemble",
    )(group, *parts)


def local(query_rows, key_rows, value_rows, query_tangent, key_tangent, value_tangent, query_gain, key_gain):
    across = lax.axis_size("head")
    blocks = lax.axis_size("blk")
    images = blocks // GROUP
    _, rows, width = query_rows.shape
    heads = width // HD
    spread = math.gcd(heads // across, GROUP)
    heads_here = heads // (across * spread)
    groups = across * spread
    copies = GROUP // spread
    low = 2 if copies % 2 == 0 else 1
    high = copies // low
    head_index = lax.axis_index("head")
    place = lax.axis_index("blk") // images
    group = (head_index * spread + (place // low) % spread).astype(jnp.int32).reshape(1)

    def moved(block, mask, far, near):
        route = []
        for h in range(across):
            for b in range(blocks):
                spot = (b // images) ^ ((far * spread + mask % spread) * low + near)
                route.append((h * blocks + b, (h ^ (mask // spread)) * blocks + spot * images + b % images))
        return lax.ppermute(block, ("head", "blk"), route)

    turn = jnp.stack(rotation((place * across + head_index) * rows, rows, HD))
    gains = jnp.stack([query_gain, key_gain])
    args = (query_rows, key_rows, value_rows, query_tangent, key_tangent, value_tangent)
    queries, keys, crossed = [], [], []
    for mask in range(groups):
        q, kv = prepare(group, mask, args, gains, turn, heads_here)
        crossed.append([moved(kv, mask, far, 0) for far in range(1, high)])
        queries.append(moved(q, mask, 0, 0) if mask else q)
        keys.append(moved(kv, mask, 0, 0) if mask else kv)

    def shared(parts):
        if low == 1:
            return parts
        return parts + [moved(p, 0, 0, 1) for p in parts]

    def joined(parts):
        if rows % 8 == 0:
            return parts
        return [jnp.concatenate(parts, axis=2)]

    queries = joined(queries)
    calls = [keys]
    for first in range(0, groups, 2):
        parts = [p for mask in range(first, min(first + 2, groups)) for p in crossed[mask]]
        if parts:
            calls.append(parts)
    state = None
    for n, parts in enumerate(calls):
        final = n == len(calls) - 1
        result = attend(queries, joined(shared(parts)), state, final, groups)
        if n == 0 and not final:
            queries = [result[0]]
            state = result[1:]
        else:
            state = result
    parts = [moved(p, mask, 0, 0) if mask else p for mask, p in enumerate(state)]
    return tuple(assemble(group, parts))


def solution(mesh):
    in_specs = (P("blk", "head", None),) * 6 + (P(), P())
    out_specs = (P("blk", "head", None), P("blk", "head", None))
    return jax.shard_map(local, mesh=mesh, in_specs=in_specs, out_specs=out_specs, check_vma=False)
```
